32 devices in a mesh: samp: 16 (over z, y, core), snp: 2 (over x).
Axes of the slice: x: 2, y: 2, z: 4, core: 2. Of those that a mesh axis runs over, the one named last changes fastest.
Arguments:
- genotypes: float32 [8192, 2048], P('samp', 'snp'), may hold values from 0 to 2, as said below
- observed: int32 [8192, 2048], P('samp', 'snp'), may hold values from 0 to 1
Outputs:
- relation: float32 [16, 2, 256, 8192], P(None, 'snp', None, 'samp')
The draws below stay inside these ranges and needn't reach their ends.
Inputs may be any that keep to these rules, and one draw needn't show every extreme that they name: `genotypes`: dosages are real numbers between 0 and 2.
All inputs are finite; a program needn't handle non-finite values.
Results may differ from the reference program's by a relative error of at most 0.00061.
Values may be sent and summed in bfloat16 or wider, within the bound.
A program may use at most 128 MiB of HBM per device.

```python
import jax
import jax.numpy as jnp
from jax import lax

SAMPLES = 8192
SNPS = 2048
TILE = 256
N_SAMP = 16
N_SNP = 2


def soft_allele(key, threshold, error_top):
    hard_key = jax.random.fold_in(key, 1)
    error_key = jax.random.fold_in(key, 2)
    carried = jax.random.uniform(hard_key, threshold.shape, jnp.float32) < threshold
    error = jax.random.uniform(error_key, threshold.shape, jnp.float32) * error_top
    return jnp.where(carried, 1.0 - error, error)


def draw_genotypes(key, part):
    rate_key = jax.random.fold_in(key, 11)
    first_key = jax.random.fold_in(key, 12)
    second_key = jax.random.fold_in(key, 13)
    base_rate = jax.random.uniform(rate_key, (SNPS,), jnp.float32, 0.005, 0.331)
    position = (jnp.arange(SAMPLES, dtype=jnp.float32) / SAMPLES)[:, None]
    threshold = base_rate[None, :] * (1.0 + 2.0 * position)
    first_allele = soft_allele(first_key, threshold, 0.3)
    second_allele = soft_allele(second_key, threshold, 0.3)
    return jnp.clip(first_allele + second_allele, 0.0, 2.0).astype(jnp.float32)


def draw_observed(key, part):
    shift_key = jax.random.fold_in(key, 21)
    call_key = jax.random.fold_in(key, 22)
    snp_shift = jax.random.randint(shift_key, (SNPS,), 0, 40)
    sample_index = jnp.arange(SAMPLES, dtype=jnp.int32)
    threshold = 500 + 480 * sample_index[:, None] // SAMPLES - snp_shift[None, :]
    call_draw = jax.random.randint(call_key, (SAMPLES, SNPS), 0, 1000)
    return (call_draw < threshold).astype(jnp.int32)


def setup_inputs(seed: int = 0) -> dict:
    key_of = jax.random.split(jax.random.key(seed), 3)
    return {
        "genotypes": draw_genotypes(jax.random.fold_in(key_of[2], 71), 0),
        "observed": draw_observed(jax.random.fold_in(key_of[2], 71), 0),
    }


var_floor = 0.1

def reference(genotypes, observed):
    present = observed.astype(jnp.float32)
    dosage = genotypes.astype(jnp.float32)
    alt_sum = lax.optimization_barrier(jnp.sum(present * dosage, axis=0))
    call_sum = lax.optimization_barrier(jnp.sum(present, axis=0))
    frequency = alt_sum / (2.0 * jnp.maximum(call_sum, 1.0))
    variance = jnp.maximum(2.0 * frequency * (1.0 - frequency), var_floor)
    scaled = (present * (dosage - 2.0 * frequency) * lax.rsqrt(variance)).astype(jnp.bfloat16)
    widened = scaled.astype(jnp.float32)
    grm = jnp.dot(widened, widened.T, precision=lax.Precision.HIGHEST) / SNPS
    return grm.reshape(N_SAMP, N_SNP, TILE, SAMPLES)
```

```python
import functools

import jax
import jax.numpy as jnp
from jax import lax
from jax.experimental import pallas as pl
from jax.experimental.pallas import tpu as pltpu
from jax.sharding import PartitionSpec as P

MESH = pl.DeviceIdType.MESH
var_floor = 0.1
UP, DOWN, SIDE, CORE = 0, 1, 2, 3
STRIP = 64


def kernel(shards, groups, geno_ref, obs_ref, out_ref, counts, panel, rows, tiles,
           count_send, count_recv, panel_send, panel_recv, row_send, row_recv, out_sem):
    row_count, snp_count = geno_ref.shape
    tile_rows = row_count // groups
    depth = shards // 4
    me = lax.axis_index("samp")
    part = lax.axis_index("snp")
    z, y, core = me // 4, (me // 2) % 2, me % 2

    def index(at_z, at_y, at_core):
        return at_z * 4 + at_y * 2 + at_core

    barrier = pltpu.get_barrier_semaphore()
    for step in range(1, shards):
        pl.semaphore_signal(barrier, inc=1, device_id={"samp": lax.rem(me + step, shards)}, device_id_type=MESH)
    for step in range(1, groups):
        pl.semaphore_signal(barrier, inc=1, device_id={"snp": lax.rem(part + step, groups)}, device_id_type=MESH)

    def add_strip(i, total):
        alt, call = total
        strip = pl.ds(pl.multiple_of(i * STRIP, STRIP), STRIP)
        present = obs_ref[strip, :].astype(jnp.float32)
        held = present * geno_ref[strip, :]
        for r in range(0, STRIP, 8):
            alt = alt + held[r:r + 8]
            call = call + present[r:r + 8]
        return alt, call

    zero = jnp.zeros((8, snp_count), jnp.float32)
    alt, call = lax.fori_loop(0, row_count // STRIP, add_strip, (zero, zero))
    counts[me, 0:1, :] = jnp.sum(alt, axis=0, keepdims=True)
    counts[me, 1:2, :] = jnp.sum(call, axis=0, keepdims=True)

    pl.semaphore_wait(barrier, shards + groups - 2)

    def count_copy(owner, to):
        return pltpu.make_async_remote_copy(
            src_ref=counts.at[owner], dst_ref=counts.at[owner], send_sem=count_send.at[to],
            recv_sem=count_recv.at[owner], device_id={"samp": to}, device_id_type=MESH)

    for step in range(1, shards):
        count_copy(me, lax.rem(me + step, shards)).start()
    for step in range(1, shards):
        other = lax.rem(me + step, shards)
        count_copy(other, other).wait_recv()
    sums = counts[0]
    for s in range(1, shards):
        sums = sums + counts[s]
    frequency = sums[0:1] / (2.0 * jnp.maximum(sums[1:2], 1.0))
    shift = 2.0 * frequency
    gain = lax.rsqrt(jnp.maximum(shift * (1.0 - frequency), var_floor))

    def panel_copy(h, k, to):
        block = panel.at[h, pl.ds(pl.multiple_of(k * tile_rows, tile_rows), tile_rows)]
        return pltpu.make_async_remote_copy(
            src_ref=block, dst_ref=block, send_sem=panel_send.at[to, k],
            recv_sem=panel_recv.at[h, k], device_id={"snp": to}, device_id_type=MESH)

    strip_rows = min(STRIP, tile_rows)

    def scale_tile(k):
        def scale_strip(i, carry):
            start = pl.multiple_of(k * tile_rows + i * strip_rows, strip_rows)
            strip = pl.ds(start, strip_rows)
            present = obs_ref[strip, :].astype(jnp.float32)
            panel[part, strip, :] = (present * (geno_ref[strip, :] - shift) * gain).astype(jnp.bfloat16)
            return carry

        lax.fori_loop(0, tile_rows // strip_rows, scale_strip, 0)

    def row_copy(q, h, way, src=None):
        to = (index(z + 1, y, core), index(z - 1, y, core), index(z, 1 - y, core), index(z, y, 1 - core))[way]
        return pltpu.make_async_remote_copy(
            src_ref=rows.at[q, h] if src is None else src, dst_ref=rows.at[q, h],
            send_sem=row_send.at[way, q, h], recv_sem=row_recv.at[q, h],
            device_id={"samp": to}, device_id_type=MESH)

    def arrive(q, h):
        row_copy(q, h, CORE).wait_recv()

    last_part = lax.rem(part + groups - 1, groups)
    turned = jnp.where(z < depth - 1, z + 1, depth - 2)

    def part_at(i):
        return lax.rem(part + i, groups)

    def source(i):
        pairs = jnp.minimum(z, depth - 1 - z)
        side = jnp.where(i % 2 == 1, z - (i + 1) // 2, z + i // 2)
        far = jnp.where(z < depth - 1 - z, z + i - pairs, z - i + pairs)
        return jnp.where(i <= 2 * pairs, side, far)

    def send_own(h):
        mine = panel.at[h, pl.ds(pl.multiple_of(part * tile_rows, tile_rows), tile_rows)]
        row_copy(me, h, SIDE, mine).start()

        @pl.when(z < depth - 1)
        def _():
            row_copy(me, h, UP, mine).start()

        @pl.when(z > 0)
        def _():
            row_copy(me, h, DOWN, mine).start()

        row_copy(me, h, CORE, mine).start()
        rows[me, h] = panel[h, pl.ds(pl.multiple_of(part * tile_rows, tile_rows), tile_rows), :]

    for step in range(1, groups):
        other = part_at(step)
        scale_tile(other)
        panel_copy(part, other, other).start()
    scale_tile(part)
    send_own(part)
    for step in range(1, groups):
        other = part_at(step)
        for k in range(1, groups):
            panel_copy(part, lax.rem(other + k, groups), other).start()
    for step in range(1, groups):
        h = part_at(step)
        panel_copy(h, part, h).wait_recv()
        send_own(h)

    def column_arrival(at_z, h, way):
        q = index(at_z, y, core)
        arrive(q, h)

        @pl.when(z < depth - 1 if way == UP else z > 0)
        def _():
            row_copy(q, h, way).start()

        @pl.when((at_z != turned) | (h != last_part))
        def _():
            row_copy(q, h, SIDE).start()

        row_copy(q, h, CORE).start()

    def column_arrivals(i):
        def per_part(t, carry):
            h = part_at(t)

            @pl.when(z - i >= 0)
            def _():
                column_arrival(z - i, h, UP)

            @pl.when(z + i < depth)
            def _():
                column_arrival(z + i, h, DOWN)

            return carry

        lax.fori_loop(0, groups, per_part, 0)

    def product(q):
        total = None
        for h in range(groups):
            term = lax.dot_general(rows[q, h], panel[h], (((1,), (1,)), ((), ())),
                                   preferred_element_type=jnp.float32)
            total = term if total is None else total + term
        tiles[q] = total * (1.0 / (groups * snp_count))
        pltpu.make_async_copy(tiles.at[q], out_ref.at[q, 0], out_sem.at[q]).start()

    def products(at_z, at_y):
        def per_core(t, carry):
            q = index(at_z, at_y, lax.rem(core + t, 2))

            @pl.when(t == 1)
            def _():
                for h in range(groups):
                    arrive(q, h)

            product(q)
            return carry

        lax.fori_loop(0, 2, per_core, 0)

    def side_arrival(at_z, h):
        q = index(at_z, 1 - y, core)
        arrive(q, h)
        row_copy(q, h, CORE).start()

    def round_of(i, carry):
        column_arrivals(i)

        @pl.when(i == 1)
        def _():
            for step in range(1, groups):
                h = part_at(step)
                for k in range(1, groups):
                    panel_copy(h, part_at(k), h).wait_recv()

        @pl.when(i == depth - 1)
        def _():
            q = index(z, 1 - y, core)

            @pl.when(z > 0)
            def _():
                row_copy(q, last_part, DOWN).start()

            @pl.when(z == depth - 2)
            def _():
                row_copy(q, last_part, UP).start()

        at_z = source(i - 1)
        products(at_z, y)

        def per_part(t, c):
            @pl.when((at_z != turned) | (t != groups - 1))
            def _():
                side_arrival(at_z, part_at(t))

            return c

        lax.fori_loop(0, groups, per_part, 0)

        @pl.when(at_z != turned)
        def _():
            products(at_z, 1 - y)

        return carry

    lax.fori_loop(1, depth + 1, round_of, 0)
    side_arrival(turned, last_part)
    products(turned, 1 - y)

    for step in range(1, shards):
        count_copy(me, lax.rem(me + step, shards)).wait_send()
    for step in range(1, groups):
        for k in range(groups):
            panel_copy(part, k, part_at(step)).wait_send()

    def drain(i, carry):
        at_z, h = i // groups, lax.rem(i, groups)
        q = index(at_z, y, core)
        across = index(at_z, 1 - y, core)

        @pl.when((at_z <= z) & (z < depth - 1))
        def _():
            row_copy(q, h, UP).wait_send()

        @pl.when((at_z >= z) & (z > 0))
        def _():
            row_copy(q, h, DOWN).wait_send()

        @pl.when((at_z != turned) | (h != last_part))
        def _():
            row_copy(q, h, SIDE).wait_send()

        row_copy(q, h, CORE).wait_send()
        row_copy(across, h, CORE).wait_send()

        @pl.when((at_z == z) & (h == last_part) & (z > 0))
        def _():
            row_copy(across, h, DOWN).wait_send()

        @pl.when((at_z == z) & (h == last_part) & (z == depth - 2))
        def _():
            row_copy(across, h, UP).wait_send()

        return carry

    lax.fori_loop(0, depth * groups, drain, 0)

    def flush(q, carry):
        pltpu.make_async_copy(tiles.at[q], out_ref.at[q, 0], out_sem.at[q]).wait()
        return carry

    lax.fori_loop(0, shards, flush, 0)


def solution(mesh):
    shards, groups = mesh.shape["samp"], mesh.shape["snp"]

    def body(genotypes, observed):
        row_count, snp_count = genotypes.shape
        tile_rows = row_count // groups
        return pl.pallas_call(
            functools.partial(kernel, shards, groups),
            out_shape=jax.ShapeDtypeStruct((shards, 1, tile_rows, row_count), jnp.float32),
            in_specs=[pl.BlockSpec(memory_space=pltpu.VMEM)] * 2,
            out_specs=pl.BlockSpec(memory_space=pl.ANY),
            scratch_shapes=[
                pltpu.VMEM((shards, 2, snp_count), jnp.float32),
                pltpu.VMEM((groups, row_count, snp_count), jnp.bfloat16),
                pltpu.VMEM((shards, groups, tile_rows, snp_count), jnp.bfloat16),
                pltpu.VMEM((shards, tile_rows, row_count), jnp.float32),
                pltpu.SemaphoreType.DMA((shards,)),
                pltpu.SemaphoreType.DMA((shards,)),
                pltpu.SemaphoreType.DMA((groups, groups)),
                pltpu.SemaphoreType.DMA((groups, groups)),
                pltpu.SemaphoreType.DMA((4, shards, groups)),
                pltpu.SemaphoreType.DMA((shards, groups)),
                pltpu.SemaphoreType.DMA((shards,)),
            ],
            compiler_params=pltpu.CompilerParams(
                collective_id=0, has_side_effects=True, vmem_limit_bytes=60 * 1024 * 1024),
        )(genotypes, observed)

    return jax.shard_map(
        body,
        mesh=mesh,
        in_specs=(P("samp", "snp"), P("samp", "snp")),
        out_specs=P(None, "snp", None, "samp"),
        check_vma=False,
    )
```

```python
import functools

import jax
import jax.numpy as jnp
from jax import lax
from jax.experimental import pallas as pl
from jax.experimental.pallas import tpu as pltpu
from jax.sharding import PartitionSpec as P

MESH = pl.DeviceIdType.MESH
var_floor = 0.1
UP, DOWN, SIDE, CORE = 0, 1, 2, 3
STRIP = 64
PIECES = 2
LOADS = 4
VMEM_ALL = 67043328
VMEM_SPARE = 512 * 1024
VMEM_FINISH = 12 * 1024 * 1024


def index(at_z, at_y, at_core):
    return at_z * 4 + at_y * 2 + at_core


def source_at(z, depth, i):
    pairs = jnp.minimum(z, depth - 1 - z)
    side = jnp.where(i % 2 == 1, z - (i + 1) // 2, z + i // 2)
    far = jnp.where(z < depth - 1 - z, z + i - pairs, z - i + pairs)
    return jnp.where(i <= 2 * pairs, side, far)


def turned_at(z, depth):
    return jnp.where(z < depth - 1, z + 1, depth - 2)


def product(rows, panel, q):
    groups, pieces, piece_rows, snp_count = rows.shape[1:]
    total = None
    for h in range(groups):
        block = rows[q, h].reshape(pieces * piece_rows, snp_count)
        term = lax.dot_general(block, panel[h], (((1,), (1,)), ((), ())), preferred_element_type=jnp.float32)
        total = term if total is None else total + term
    return total * (1.0 / (groups * snp_count))


def finish(shards, groups, rows, panel, tiles, out_ref, late, out_sem):
    depth = shards // 4
    me = lax.axis_index("samp")
    z, y = me // 4, (me // 2) % 2
    turned = turned_at(z, depth)
    final = source_at(z, depth, depth - 1)
    final = jnp.where(final == turned, source_at(z, depth, depth - 2), final)

    def is_late(q):
        return ((q // 4 == turned) | (q // 4 == final)) & ((q // 2) % 2 != y)

    def put(q, carry):
        @pl.when(jnp.logical_not(is_late(q)))
        def _():
            pltpu.make_async_copy(tiles.at[q], out_ref.at[q, 0], out_sem.at[q]).start()

        return carry

    lax.fori_loop(0, shards, put, 0)

    def form(i, carry):
        q = index(jnp.where(i // 2 == 0, final, turned), 1 - y, lax.rem(i, 2))
        late[i] = product(rows, panel, q)
        pltpu.make_async_copy(late.at[i], out_ref.at[q, 0], out_sem.at[q]).start()
        return carry

    lax.fori_loop(0, 4, form, 0)

    def flush(q, carry):
        pltpu.make_async_copy(tiles.at[q], out_ref.at[q, 0], out_sem.at[q]).wait()
        return carry

    lax.fori_loop(0, shards, flush, 0)


def kernel(shards, groups, geno_hbm, obs_hbm, panel, rows, tiles, geno_ref, obs_ref, counts, load_sem,
           count_send, count_recv, panel_send, panel_recv, row_send, row_recv):
    row_count, snp_count = geno_ref.shape
    tile_rows = row_count // groups
    piece_rows = tile_rows // PIECES
    depth = shards // 4
    me = lax.axis_index("samp")
    part = lax.axis_index("snp")
    z, y, core = me // 4, (me // 2) % 2, me % 2

    load_rows = row_count // LOADS

    def load(i):
        block = pl.ds(pl.multiple_of(i * load_rows, load_rows), load_rows)
        return (pltpu.make_async_copy(geno_hbm.at[block], geno_ref.at[block], load_sem.at[0, i]),
                pltpu.make_async_copy(obs_hbm.at[block], obs_ref.at[block], load_sem.at[1, i]))

    for i in range(LOADS):
        for copy in load(i):
            copy.start()

    barrier = pltpu.get_barrier_semaphore()
    for step in range(1, shards):
        pl.semaphore_signal(barrier, inc=1, device_id={"samp": lax.rem(me + step, shards)}, device_id_type=MESH)
    for step in range(1, groups):
        pl.semaphore_signal(barrier, inc=1, device_id={"snp": lax.rem(part + step, groups)}, device_id_type=MESH)

    def add_strip(i, total):
        alt, call = total
        strip = pl.ds(pl.multiple_of(i * STRIP, STRIP), STRIP)
        present = obs_ref[strip, :].astype(jnp.float32)
        held = present * geno_ref[strip, :]
        for r in range(0, STRIP, 8):
            alt = alt + held[r:r + 8]
            call = call + present[r:r + 8]
        return alt, call

    zero = jnp.zeros((8, snp_count), jnp.float32)
    alt, call = zero, zero
    strips = load_rows // STRIP
    for i in range(LOADS):
        for copy in load(i):
            copy.wait()
        alt, call = lax.fori_loop(i * strips, (i + 1) * strips, add_strip, (alt, call))
    counts[me, 0:1, :] = jnp.sum(alt, axis=0, keepdims=True)
    counts[me, 1:2, :] = jnp.sum(call, axis=0, keepdims=True)

    pl.semaphore_wait(barrier, shards + groups - 2)

    def count_copy(owner, to):
        return pltpu.make_async_remote_copy(
            src_ref=counts.at[owner], dst_ref=counts.at[owner], send_sem=count_send.at[to],
            recv_sem=count_recv.at[owner], device_id={"samp": to}, device_id_type=MESH)

    for step in range(1, shards):
        count_copy(me, lax.rem(me + step, shards)).start()
    for step in range(1, shards):
        other = lax.rem(me + step, shards)
        count_copy(other, other).wait_recv()
    sums = counts[0]
    for s in range(1, shards):
        sums = sums + counts[s]
    frequency = sums[0:1] / (2.0 * jnp.maximum(sums[1:2], 1.0))
    shift = 2.0 * frequency
    gain = lax.rsqrt(jnp.maximum(shift * (1.0 - frequency), var_floor))

    def piece_of(k, p):
        return pl.ds(pl.multiple_of(k * tile_rows + p * piece_rows, piece_rows), piece_rows)

    def panel_copy(h, k, to, p):
        block = panel.at[h, piece_of(k, p)]
        return pltpu.make_async_remote_copy(
            src_ref=block, dst_ref=block, send_sem=panel_send.at[to, k, p],
            recv_sem=panel_recv.at[h, k, p], device_id={"snp": to}, device_id_type=MESH)

    strip_rows = min(STRIP, piece_rows)

    def scale_piece(k, p):
        def scale_strip(i, carry):
            start = pl.multiple_of(k * tile_rows + p * piece_rows + i * strip_rows, strip_rows)
            strip = pl.ds(start, strip_rows)
            present = obs_ref[strip, :].astype(jnp.float32)
            panel[part, strip, :] = (present * (geno_ref[strip, :] - shift) * gain).astype(jnp.bfloat16)
            return carry

        lax.fori_loop(0, piece_rows // strip_rows, scale_strip, 0)

    def row_copy(q, h, p, way, src=None):
        to = (index(z + 1, y, core), index(z - 1, y, core), index(z, 1 - y, core), index(z, y, 1 - core))[way]
        return pltpu.make_async_remote_copy(
            src_ref=rows.at[q, h, p] if src is None else src, dst_ref=rows.at[q, h, p],
            send_sem=row_send.at[way, q, h, p], recv_sem=row_recv.at[q, h, p],
            device_id={"samp": to}, device_id_type=MESH)

    def arrive(q, h, p):
        row_copy(q, h, p, CORE).wait_recv()

    last_part = lax.rem(part + groups - 1, groups)
    turned = turned_at(z, depth)

    def part_at(i):
        return lax.rem(part + i, groups)

    def send_own(h, p):
        mine = panel.at[h, piece_of(part, p)]
        row_copy(me, h, p, SIDE, mine).start()

        @pl.when(z < depth - 1)
        def _():
            row_copy(me, h, p, UP, mine).start()

        @pl.when(z > 0)
        def _():
            row_copy(me, h, p, DOWN, mine).start()

        row_copy(me, h, p, CORE, mine).start()
        rows[me, h, p] = panel[h, piece_of(part, p), :]

    for p in range(PIECES):
        for step in range(1, groups):
            other = part_at(step)
            scale_piece(other, p)
            panel_copy(part, other, other, p).start()
        scale_piece(part, p)
        send_own(part, p)
    for step in range(1, groups):
        other = part_at(step)
        for k in range(1, groups):
            for p in range(PIECES):
                panel_copy(part, lax.rem(other + k, groups), other, p).start()
    for step in range(1, groups):
        h = part_at(step)
        for p in range(PIECES):
            panel_copy(h, part, h, p).wait_recv()
            send_own(h, p)

    def column_arrival(at_z, h, p, way):
        q = index(at_z, y, core)
        arrive(q, h, p)

        @pl.when(z < depth - 1 if way == UP else z > 0)
        def _():
            row_copy(q, h, p, way).start()

        @pl.when((at_z != turned) | (h != last_part))
        def _():
            row_copy(q, h, p, SIDE).start()

        row_copy(q, h, p, CORE).start()

    def column_arrivals(i):
        def per_piece(t, carry):
            h, p = part_at(t // PIECES), lax.rem(t, PIECES)

            @pl.when(z - i >= 0)
            def _():
                column_arrival(z - i, h, p, UP)

            @pl.when(z + i < depth)
            def _():
                column_arrival(z + i, h, p, DOWN)

            return carry

        lax.fori_loop(0, groups * PIECES, per_piece, 0)

    def arrive_all(q):
        def per_piece(t, carry):
            arrive(q, t // PIECES, lax.rem(t, PIECES))
            return carry

        lax.fori_loop(0, groups * PIECES, per_piece, 0)

    def products(at_z, at_y):
        def per_core(t, carry):
            q = index(at_z, at_y, lax.rem(core + t, 2))

            @pl.when(t == 1)
            def _():
                arrive_all(q)

            tiles[q] = product(rows, panel, q)
            return carry

        lax.fori_loop(0, 2, per_core, 0)

    def side_arrival(at_z, h, p):
        q = index(at_z, 1 - y, core)
        arrive(q, h, p)
        row_copy(q, h, p, CORE).start()

    final = source_at(z, depth, depth - 1)
    final = jnp.where(final == turned, source_at(z, depth, depth - 2), final)

    def round_of(i, carry):
        @pl.when(i < depth)
        def _():
            column_arrivals(i)

        @pl.when(i == 1)
        def _():
            for step in range(1, groups):
                h = part_at(step)
                for k in range(1, groups):
                    for p in range(PIECES):
                        panel_copy(h, part_at(k), h, p).wait_recv()

        @pl.when(i == depth - 1)
        def _():
            q = index(z, 1 - y, core)

            @pl.when(z > 0)
            def _():
                for p in range(PIECES):
                    row_copy(q, last_part, p, DOWN).start()

            @pl.when(z == depth - 2)
            def _():
                for p in range(PIECES):
                    row_copy(q, last_part, p, UP).start()

        at_z = source_at(z, depth, i - 1)
        products(at_z, y)

        def per_piece(t, c):
            @pl.when((at_z != turned) | (t // PIECES != groups - 1))
            def _():
                side_arrival(at_z, part_at(t // PIECES), lax.rem(t, PIECES))

            return c

        lax.fori_loop(0, groups * PIECES, per_piece, 0)

        @pl.when((at_z != turned) & (at_z != final))
        def _():
            products(at_z, 1 - y)

        return carry

    lax.fori_loop(1, depth + 1, round_of, 0)
    for p in range(PIECES):
        side_arrival(turned, last_part, p)
    arrive_all(index(final, 1 - y, 1 - core))
    arrive_all(index(turned, 1 - y, 1 - core))

    for step in range(1, shards):
        count_copy(me, lax.rem(me + step, shards)).wait_send()
    for step in range(1, groups):
        for k in range(groups):
            for p in range(PIECES):
                panel_copy(part, k, part_at(step), p).wait_send()

    def drain(i, carry):
        at_z, h, p = i // (groups * PIECES), lax.rem(i // PIECES, groups), lax.rem(i, PIECES)
        q = index(at_z, y, core)
        across = index(at_z, 1 - y, core)

        @pl.when((at_z <= z) & (z < depth - 1))
        def _():
            row_copy(q, h, p, UP).wait_send()

        @pl.when((at_z >= z) & (z > 0))
        def _():
            row_copy(q, h, p, DOWN).wait_send()

        @pl.when((at_z != turned) | (h != last_part))
        def _():
            row_copy(q, h, p, SIDE).wait_send()

        row_copy(q, h, p, CORE).wait_send()
        row_copy(across, h, p, CORE).wait_send()

        @pl.when((at_z == z) & (h == last_part) & (z > 0))
        def _():
            row_copy(across, h, p, DOWN).wait_send()

        @pl.when((at_z == z) & (h == last_part) & (z == depth - 2))
        def _():
            row_copy(across, h, p, UP).wait_send()

        return carry

    lax.fori_loop(0, depth * groups * PIECES, drain, 0)


def solution(mesh):
    shards, groups = mesh.shape["samp"], mesh.shape["snp"]

    def body(genotypes, observed):
        row_count, snp_count = genotypes.shape
        tile_rows = row_count // groups
        piece_rows = tile_rows // PIECES
        kept = 2 * (groups * row_count * snp_count) * (1 + shards // groups) + 4 * shards * tile_rows * row_count
        panel, rows, tiles = pl.pallas_call(
            functools.partial(kernel, shards, groups),
            out_shape=(
                pltpu.VMEM((groups, row_count, snp_count), jnp.bfloat16),
                pltpu.VMEM((shards, groups, PIECES, piece_rows, snp_count), jnp.bfloat16),
                pltpu.VMEM((shards, tile_rows, row_count), jnp.float32),
            ),
            in_specs=[pl.BlockSpec(memory_space=pltpu.HBM)] * 2,
            out_specs=[pl.BlockSpec(memory_space=pltpu.VMEM)] * 3,
            scratch_shapes=[
                pltpu.VMEM((row_count, snp_count), jnp.float32),
                pltpu.VMEM((row_count, snp_count), jnp.int32),
                pltpu.VMEM((shards, 2, snp_count), jnp.float32),
                pltpu.SemaphoreType.DMA((2, LOADS)),
                pltpu.SemaphoreType.DMA((shards,)),
                pltpu.SemaphoreType.DMA((shards,)),
                pltpu.SemaphoreType.DMA((groups, groups, PIECES)),
                pltpu.SemaphoreType.DMA((groups, groups, PIECES)),
                pltpu.SemaphoreType.DMA((4, shards, groups, PIECES)),
                pltpu.SemaphoreType.DMA((shards, groups, PIECES)),
            ],
            compiler_params=pltpu.CompilerParams(
                collective_id=0, has_side_effects=True, vmem_limit_bytes=VMEM_ALL - VMEM_SPARE - kept),
        )(genotypes, observed)
        return pl.pallas_call(
            functools.partial(finish, shards, groups),
            out_shape=jax.ShapeDtypeStruct((shards, 1, tile_rows, row_count), jnp.float32),
            in_specs=[pl.BlockSpec(memory_space=pltpu.VMEM)] * 3,
            out_specs=pl.BlockSpec(memory_space=pltpu.HBM),
            scratch_shapes=[
                pltpu.VMEM((4, tile_rows, row_count), jnp.float32),
                pltpu.SemaphoreType.DMA((shards,)),
            ],
            compiler_params=pltpu.CompilerParams(vmem_limit_bytes=VMEM_FINISH),
        )(rows, panel, tiles)

    return jax.shard_map(
        body,
        mesh=mesh,
        in_specs=(P("samp", "snp"), P("samp", "snp")),
        out_specs=P(None, "snp", None, "samp"),
        check_vma=False,
    )
```

```python
import functools

import jax
import jax.numpy as jnp
from jax import lax
from jax.experimental import pallas as pl
from jax.experimental.pallas import tpu as pltpu
from jax.sharding import PartitionSpec as P

MESH = pl.DeviceIdType.MESH
var_floor = 0.1
UP, DOWN, SIDE, CORE = 0, 1, 2, 3
STRIP = 64
PIECES = 2
LOADS = 4
VMEM_ALL = 67043328
VMEM_SPARE = 512 * 1024
VMEM_FINISH = 12 * 1024 * 1024


def index(at_z, at_y, at_core):
    return at_z * 4 + at_y * 2 + at_core


def source_at(z, depth, i):
    pairs = jnp.minimum(z, depth - 1 - z)
    side = jnp.where(i % 2 == 1, z - (i + 1) // 2, z + i // 2)
    far = jnp.where(z < depth - 1 - z, z + i - pairs, z - i + pairs)
    return jnp.where(i <= 2 * pairs, side, far)


def turned_at(z, depth):
    return jnp.where(z < depth - 1, z + 1, depth - 2)


def product(rows, panel, q, parts):
    pieces, piece_rows, snp_count = rows.shape[2:]
    total = None
    for h in parts:
        block = rows[q, h].reshape(pieces * piece_rows, snp_count)
        term = lax.dot_general(block, panel[h], (((1,), (1,)), ((), ())), preferred_element_type=jnp.float32)
        total = term if total is None else total + term
    return total * (1.0 / (rows.shape[1] * snp_count))


def finish(shards, groups, rows, panel, tiles, out_ref, late, out_sem):
    depth = shards // 4
    me = lax.axis_index("samp")
    z, y = me // 4, (me // 2) % 2
    turned = turned_at(z, depth)
    final = source_at(z, depth, depth - 1)
    final = jnp.where(final == turned, source_at(z, depth, depth - 2), final)
    last_part = lax.rem(lax.axis_index("snp") + groups - 1, groups)

    def is_late(q):
        return ((q // 4 == turned) | (q // 4 == final)) & ((q // 2) % 2 != y)

    def put(q, carry):
        @pl.when(jnp.logical_not(is_late(q)))
        def _():
            pltpu.make_async_copy(tiles.at[q], out_ref.at[q, 0], out_sem.at[q]).start()

        return carry

    lax.fori_loop(0, shards, put, 0)

    def form(i, carry):
        q = index(jnp.where(i // 2 == 0, final, turned), 1 - y, lax.rem(i, 2))
        late[i] = tiles[q] + product(rows, panel, q, [last_part])
        pltpu.make_async_copy(late.at[i], out_ref.at[q, 0], out_sem.at[q]).start()
        return carry

    lax.fori_loop(0, 4, form, 0)

    def flush(q, carry):
        pltpu.make_async_copy(tiles.at[q], out_ref.at[q, 0], out_sem.at[q]).wait()
        return carry

    lax.fori_loop(0, shards, flush, 0)


def kernel(shards, groups, geno_hbm, obs_hbm, panel, rows, tiles, geno_ref, obs_ref, counts, load_sem,
           count_send, count_recv, panel_send, panel_recv, row_send, row_recv):
    row_count, snp_count = geno_ref.shape
    tile_rows = row_count // groups
    piece_rows = tile_rows // PIECES
    depth = shards // 4
    me = lax.axis_index("samp")
    part = lax.axis_index("snp")
    z, y, core = me // 4, (me // 2) % 2, me % 2

    load_rows = row_count // LOADS

    def load(i):
        block = pl.ds(pl.multiple_of(i * load_rows, load_rows), load_rows)
        return (pltpu.make_async_copy(geno_hbm.at[block], geno_ref.at[block], load_sem.at[0, i]),
                pltpu.make_async_copy(obs_hbm.at[block], obs_ref.at[block], load_sem.at[1, i]))

    for i in range(LOADS):
        for copy in load(i):
            copy.start()

    barrier = pltpu.get_barrier_semaphore()
    for step in range(1, shards):
        pl.semaphore_signal(barrier, inc=1, device_id={"samp": lax.rem(me + step, shards)}, device_id_type=MESH)
    for step in range(1, groups):
        pl.semaphore_signal(barrier, inc=1, device_id={"snp": lax.rem(part + step, groups)}, device_id_type=MESH)

    def add_strip(i, total):
        alt, call = total
        strip = pl.ds(pl.multiple_of(i * STRIP, STRIP), STRIP)
        present = obs_ref[strip, :].astype(jnp.float32)
        held = present * geno_ref[strip, :]
        for r in range(0, STRIP, 8):
            alt = alt + held[r:r + 8]
            call = call + present[r:r + 8]
        return alt, call

    zero = jnp.zeros((8, snp_count), jnp.float32)
    alt, call = zero, zero
    strips = load_rows // STRIP
    for i in range(LOADS):
        for copy in load(i):
            copy.wait()
        alt, call = lax.fori_loop(i * strips, (i + 1) * strips, add_strip, (alt, call))
    counts[me, 0:1, :] = jnp.sum(alt, axis=0, keepdims=True)
    counts[me, 1:2, :] = jnp.sum(call, axis=0, keepdims=True)

    pl.semaphore_wait(barrier, shards + groups - 2)

    def count_copy(owner, to):
        return pltpu.make_async_remote_copy(
            src_ref=counts.at[owner], dst_ref=counts.at[owner], send_sem=count_send.at[to],
            recv_sem=count_recv.at[owner], device_id={"samp": to}, device_id_type=MESH)

    for step in range(1, shards):
        count_copy(me, lax.rem(me + step, shards)).start()
    for step in range(1, shards):
        other = lax.rem(me + step, shards)
        count_copy(other, other).wait_recv()
    sums = counts[0]
    for s in range(1, shards):
        sums = sums + counts[s]
    frequency = sums[0:1] / (2.0 * jnp.maximum(sums[1:2], 1.0))
    shift = 2.0 * frequency
    gain = lax.rsqrt(jnp.maximum(shift * (1.0 - frequency), var_floor))

    def piece_of(k, p):
        return pl.ds(pl.multiple_of(k * tile_rows + p * piece_rows, piece_rows), piece_rows)

    def panel_copy(h, k, to, p):
        block = panel.at[h, piece_of(k, p)]
        return pltpu.make_async_remote_copy(
            src_ref=block, dst_ref=block, send_sem=panel_send.at[to, k, p],
            recv_sem=panel_recv.at[h, k, p], device_id={"snp": to}, device_id_type=MESH)

    strip_rows = min(STRIP, piece_rows)

    def scale_piece(k, p):
        def scale_strip(i, carry):
            start = pl.multiple_of(k * tile_rows + p * piece_rows + i * strip_rows, strip_rows)
            strip = pl.ds(start, strip_rows)
            present = obs_ref[strip, :].astype(jnp.float32)
            panel[part, strip, :] = (present * (geno_ref[strip, :] - shift) * gain).astype(jnp.bfloat16)
            return carry

        lax.fori_loop(0, piece_rows // strip_rows, scale_strip, 0)

    def row_copy(q, h, p, way, src=None):
        to = (index(z + 1, y, core), index(z - 1, y, core), index(z, 1 - y, core), index(z, y, 1 - core))[way]
        return pltpu.make_async_remote_copy(
            src_ref=rows.at[q, h, p] if src is None else src, dst_ref=rows.at[q, h, p],
            send_sem=row_send.at[way, q, h, p], recv_sem=row_recv.at[q, h, p],
            device_id={"samp": to}, device_id_type=MESH)

    def arrive(q, h, p):
        row_copy(q, h, p, CORE).wait_recv()

    last_part = lax.rem(part + groups - 1, groups)
    turned = turned_at(z, depth)

    def part_at(i):
        return lax.rem(part + i, groups)

    def send_own(h, p):
        mine = panel.at[h, piece_of(part, p)]
        row_copy(me, h, p, SIDE, mine).start()

        @pl.when(z < depth - 1)
        def _():
            row_copy(me, h, p, UP, mine).start()

        @pl.when(z > 0)
        def _():
            row_copy(me, h, p, DOWN, mine).start()

        row_copy(me, h, p, CORE, mine).start()
        rows[me, h, p] = panel[h, piece_of(part, p), :]

    for p in range(PIECES):
        for step in range(1, groups):
            other = part_at(step)
            scale_piece(other, p)
            panel_copy(part, other, other, p).start()
        scale_piece(part, p)
        send_own(part, p)
    for step in range(1, groups):
        other = part_at(step)
        for k in range(1, groups):
            for p in range(PIECES):
                panel_copy(part, lax.rem(other + k, groups), other, p).start()
    for step in range(1, groups):
        h = part_at(step)
        for p in range(PIECES):
            panel_copy(h, part, h, p).wait_recv()
            send_own(h, p)

    def column_arrival(at_z, h, p, way):
        q = index(at_z, y, core)
        arrive(q, h, p)

        @pl.when(z < depth - 1 if way == UP else z > 0)
        def _():
            row_copy(q, h, p, way).start()

        @pl.when((at_z != turned) | (h != last_part))
        def _():
            row_copy(q, h, p, SIDE).start()

        row_copy(q, h, p, CORE).start()

    def column_arrivals(i):
        def per_piece(t, carry):
            h, p = part_at(t // PIECES), lax.rem(t, PIECES)

            @pl.when(z - i >= 0)
            def _():
                column_arrival(z - i, h, p, UP)

            @pl.when(z + i < depth)
            def _():
                column_arrival(z + i, h, p, DOWN)

            return carry

        lax.fori_loop(0, groups * PIECES, per_piece, 0)

    def arrive_all(q):
        def per_piece(t, carry):
            arrive(q, t // PIECES, lax.rem(t, PIECES))
            return carry

        lax.fori_loop(0, groups * PIECES, per_piece, 0)

    def products(at_z, at_y):
        def per_core(t, carry):
            q = index(at_z, at_y, lax.rem(core + t, 2))

            @pl.when(t == 1)
            def _():
                arrive_all(q)

            tiles[q] = product(rows, panel, q, range(groups))
            return carry

        lax.fori_loop(0, 2, per_core, 0)

    def side_arrival(at_z, h, p):
        q = index(at_z, 1 - y, core)
        arrive(q, h, p)
        row_copy(q, h, p, CORE).start()

    final = source_at(z, depth, depth - 1)
    final = jnp.where(final == turned, source_at(z, depth, depth - 2), final)

    def begin_late():
        def per_tile(t, carry):
            q = index(jnp.where(t % 2 == 0, turned, final), 1 - y, lax.rem(core + t // 2, 2))

            @pl.when(t >= 2)
            def _():
                for step in range(groups - 1):
                    for p in range(PIECES):
                        arrive(q, part_at(step), p)

            tiles[q] = product(rows, panel, q, [part_at(step) for step in range(groups - 1)])
            return carry

        lax.fori_loop(0, 4, per_tile, 0)

    def round_of(i, carry):
        @pl.when(i < depth)
        def _():
            column_arrivals(i)

        @pl.when(i == 1)
        def _():
            for step in range(1, groups):
                h = part_at(step)
                for k in range(1, groups):
                    for p in range(PIECES):
                        panel_copy(h, part_at(k), h, p).wait_recv()

        @pl.when(i == depth - 1)
        def _():
            q = index(z, 1 - y, core)

            @pl.when(z > 0)
            def _():
                for p in range(PIECES):
                    row_copy(q, last_part, p, DOWN).start()

            @pl.when(z == depth - 2)
            def _():
                for p in range(PIECES):
                    row_copy(q, last_part, p, UP).start()

        at_z = source_at(z, depth, i - 1)
        products(at_z, y)

        def per_piece(t, c):
            @pl.when((i == depth) & (t == (groups - 1) * PIECES))
            def _():
                begin_late()

            @pl.when((at_z != turned) | (t // PIECES != groups - 1))
            def _():
                side_arrival(at_z, part_at(t // PIECES), lax.rem(t, PIECES))

            return c

        lax.fori_loop(0, groups * PIECES, per_piece, 0)

        @pl.when((at_z != turned) & (at_z != final))
        def _():
            products(at_z, 1 - y)

        return carry

    lax.fori_loop(1, depth + 1, round_of, 0)
    for p in range(PIECES):
        side_arrival(turned, last_part, p)
    for p in range(PIECES):
        arrive(index(final, 1 - y, 1 - core), last_part, p)
        arrive(index(turned, 1 - y, 1 - core), last_part, p)

    for step in range(1, shards):
        count_copy(me, lax.rem(me + step, shards)).wait_send()
    for step in range(1, groups):
        for k in range(groups):
            for p in range(PIECES):
                panel_copy(part, k, part_at(step), p).wait_send()

    def drain(i, carry):
        at_z, h, p = i // (groups * PIECES), lax.rem(i // PIECES, groups), lax.rem(i, PIECES)
        q = index(at_z, y, core)
        across = index(at_z, 1 - y, core)

        @pl.when((at_z <= z) & (z < depth - 1))
        def _():
            row_copy(q, h, p, UP).wait_send()

        @pl.when((at_z >= z) & (z > 0))
        def _():
            row_copy(q, h, p, DOWN).wait_send()

        @pl.when((at_z != turned) | (h != last_part))
        def _():
            row_copy(q, h, p, SIDE).wait_send()

        row_copy(q, h, p, CORE).wait_send()
        row_copy(across, h, p, CORE).wait_send()

        @pl.when((at_z == z) & (h == last_part) & (z > 0))
        def _():
            row_copy(across, h, p, DOWN).wait_send()

        @pl.when((at_z == z) & (h == last_part) & (z == depth - 2))
        def _():
            row_copy(across, h, p, UP).wait_send()

        return carry

    lax.fori_loop(0, depth * groups * PIECES, drain, 0)


def solution(mesh):
    shards, groups = mesh.shape["samp"], mesh.shape["snp"]

    def body(genotypes, observed):
        row_count, snp_count = genotypes.shape
        tile_rows = row_count // groups
        piece_rows = tile_rows // PIECES
        kept = 2 * (groups * row_count * snp_count) * (1 + shards // groups) + 4 * shards * tile_rows * row_count
        panel, rows, tiles = pl.pallas_call(
            functools.partial(kernel, shards, groups),
            out_shape=(
                pltpu.VMEM((groups, row_count, snp_count), jnp.bfloat16),
                pltpu.VMEM((shards, groups, PIECES, piece_rows, snp_count), jnp.bfloat16),
                pltpu.VMEM((shards, tile_rows, row_count), jnp.float32),
            ),
            in_specs=[pl.BlockSpec(memory_space=pltpu.HBM)] * 2,
            out_specs=[pl.BlockSpec(memory_space=pltpu.VMEM)] * 3,
            scratch_shapes=[
                pltpu.VMEM((row_count, snp_count), jnp.float32),
                pltpu.VMEM((row_count, snp_count), jnp.int32),
                pltpu.VMEM((shards, 2, snp_count), jnp.float32),
                pltpu.SemaphoreType.DMA((2, LOADS)),
                pltpu.SemaphoreType.DMA((shards,)),
                pltpu.SemaphoreType.DMA((shards,)),
                pltpu.SemaphoreType.DMA((groups, groups, PIECES)),
                pltpu.SemaphoreType.DMA((groups, groups, PIECES)),
                pltpu.SemaphoreType.DMA((4, shards, groups, PIECES)),
                pltpu.SemaphoreType.DMA((shards, groups, PIECES)),
            ],
            compiler_params=pltpu.CompilerParams(
                collective_id=0, has_side_effects=True, vmem_limit_bytes=VMEM_ALL - VMEM_SPARE - kept),
        )(genotypes, observed)
        return pl.pallas_call(
            functools.partial(finish, shards, groups),
            out_shape=jax.ShapeDtypeStruct((shards, 1, tile_rows, row_count), jnp.float32),
            in_specs=[pl.BlockSpec(memory_space=pltpu.VMEM)] * 3,
            out_specs=pl.BlockSpec(memory_space=pltpu.HBM),
            scratch_shapes=[
                pltpu.VMEM((4, tile_rows, row_count), jnp.float32),
                pltpu.SemaphoreType.DMA((shards,)),
            ],
            compiler_params=pltpu.CompilerParams(vmem_limit_bytes=VMEM_FINISH),
        )(rows, panel, tiles)

    return jax.shard_map(
        body,
        mesh=mesh,
        in_specs=(P("samp", "snp"), P("samp", "snp")),
        out_specs=P(None, "snp", None, "samp"),
        check_vma=False,
    )
```
